32 devices in a mesh: ctx: 16 (over z, x, core), head: 2 (over y).
Axes of the slice: x: 2, y: 2, z: 4, core: 2. Of those that a mesh axis runs over, the one named last changes fastest.
Arguments:
- queries: bfloat16 [8192, 16, 128], P('ctx', 'head'), may hold values from -160 to 160, as said below
- keys: bfloat16 [8192, 2, 128], P('ctx', 'head'), may hold values from -4 to 4
- values: bfloat16 [8192, 2, 128], P('ctx', 'head'), may hold values from -6 to 6
- doc_lengths: int32 [32], replicated, may hold values from 1 to 4096, 8192 in all
Outputs:
- attended: bfloat16 [8192, 2048], P(('ctx', 'head'))
The draws below stay inside these ranges and needn't reach their ends.
Inputs may be any that keep to these rules, and one draw needn't show every extreme that they name: `queries`: queries of several heads for a few tokens may be large multiples of sums of earlier keys of the same key head. `doc_lengths`: the lengths sum to 8192; the largest is exactly 4096.
All inputs are finite; a program needn't handle non-finite values.
Results may differ from the reference program's by a relative error of at most 0.0033.
Values may be sent and summed in bfloat16 or wider, within the bound.
A program may use at most 64 MiB of HBM per device.

```python
import math
import jax
import jax.numpy as jnp
import numpy as np
from jax import lax

HD = 128
TOK_DEV = 512
SPAN = 8
KV_HEADS = 2
QH = 16
TOKENS = 8192
DOCS = 32
DOC_MOST = 4096


def make_pair(key):
    key_keys = jax.random.fold_in(key, 11)
    key_queries = jax.random.fold_in(key, 23)
    key_vectors = jnp.clip(jax.random.normal(key_keys, (TOKENS, KV_HEADS, HD), jnp.float32), -4.0, 4.0)
    query_vectors = jnp.clip(jax.random.normal(key_queries, (TOKENS, QH, HD), jnp.float32), -6.0, 6.0)
    return (query_vectors, key_vectors)


def draw_queries(key, part):
    return make_pair(key)[0].astype(jnp.bfloat16)


def draw_keys(key, part):
    return make_pair(key)[1].astype(jnp.bfloat16)


def shard_levels(key, extent, shards, least, high):
    def one(dim, parts):
        heights = jax.random.uniform(jax.random.fold_in(jax.random.fold_in(key, 6), dim), (parts,), jnp.float32, least / len(shards), high / len(shards))
        return jnp.repeat(jnp.exp(heights), extent[dim] // parts).reshape((-1,) + (1,) * (len(extent) - dim - 1))

    gain = one(*shards[0])
    for cut in shards[1:]:
        gain = gain * one(*cut)
    return gain


def split_up(number_of, total, bound, lean):
    portions = [(1 << 20) // math.isqrt(grade ** lean) + 1 for grade in range(2, number_of + 1)]
    rest, counts = total - bound - (number_of - 1), [1] * (number_of - 1)
    while rest > 0:
        candidates = [i for i in range(number_of - 1) if counts[i] < bound]
        pool, left = sum([portions[i] for i in candidates]), rest
        for i in candidates:
            extra = min(bound - counts[i], max(1, left * portions[i] // pool), rest)
            counts[i] = counts[i] + extra
            rest = rest - extra
    return np.array([bound] + counts)


def ragged_sizes(rng, amount, total, limit, slope):
    if amount == 2:
        one = jax.random.randint(rng, (), max(1, total - limit), min(limit, total - 1) + 1)
        return jnp.stack([one, total - one])
    tallies = jnp.asarray(split_up(amount, total, limit, slope), jnp.int32)
    pairs = (amount - 1) // 2
    source_of, receiver = tallies[1:1 + 2 * pairs:2], tallies[2:2 + 2 * pairs:2]
    slack = jnp.minimum(source_of - 1, limit - receiver)
    passed = jax.random.randint(jax.random.fold_in(rng, 1), (pairs,), 0, 1 << 20) % (slack + 1)
    tallies = tallies.at[1:1 + 2 * pairs:2].set(source_of - passed).at[2:2 + 2 * pairs:2].set(receiver + passed)
    return tallies[jax.random.permutation(jax.random.fold_in(rng, 2), amount)]


def noise(key, extent, width, most, shards=(), kind=jnp.bfloat16):
    level = shard_levels(key, extent, shards, -0.22, 0.18) if shards else 1.0
    values = jax.random.normal(key, extent, jnp.float32) * width * level
    return jnp.minimum(jnp.maximum(values, -most), most).astype(kind)


def setup_inputs(seed: int = 0) -> dict:
    arg_keys = jax.random.split(jax.random.key(seed), 5)
    queries = draw_queries(jax.random.fold_in(arg_keys[4], 71), 0)
    keys = draw_keys(jax.random.fold_in(arg_keys[4], 71), 0)
    values = noise(arg_keys[2], (TOKENS, KV_HEADS, HD), 1.0, 6.0, ((0, 16), (1, 2)))
    doc_lengths = ragged_sizes(arg_keys[3], DOCS, TOKENS, DOC_MOST, 2).astype(jnp.int32)
    return {"queries": queries, "keys": keys, "values": values, "doc_lengths": doc_lengths}


def doc_index(positions, ends):
    return jnp.sum((ends[None, :] <= positions[:, None]).astype(jnp.int32), axis=1).astype(jnp.int32)


def reference(queries, keys, values, doc_lengths):
    tokens, qheads, hdim = queries.shape
    kvheads = keys.shape[1]
    group = qheads // kvheads
    block = TOK_DEV
    scale = 1.0 / (hdim ** 0.5)
    ends = jnp.cumsum(doc_lengths).astype(jnp.int32)
    docs = doc_index(jnp.arange(tokens, dtype=jnp.int32), ends)
    front = jnp.zeros((SPAN * block, kvheads, hdim), keys.dtype)
    key_pad = jnp.concatenate([front, keys], axis=0)
    value_pad = jnp.concatenate([front, values], axis=0)
    grouped = queries.reshape(tokens, kvheads, group, hdim)

    def one_block(index):
        start = (index * block).astype(jnp.int32)
        query_block = lax.dynamic_slice_in_dim(grouped, start, block, 0).astype(jnp.float32)
        qpos = start + jnp.arange(block, dtype=jnp.int32)
        qdoc = lax.dynamic_slice_in_dim(docs, start, block, 0)

        def update(state, back):
            first = (start - back * block).astype(jnp.int32)
            key_block = lax.dynamic_slice_in_dim(key_pad, first + SPAN * block, block, 0).astype(jnp.float32)
            value_block = lax.dynamic_slice_in_dim(value_pad, first + SPAN * block, block, 0).astype(jnp.float32)
            kpos = first + jnp.arange(block, dtype=jnp.int32)
            kdoc = doc_index(jnp.maximum(kpos, 0), ends)
            mask = (kdoc[None, :] == qdoc[:, None]) & (kpos[None, :] <= qpos[:, None]) & (kpos[None, :] >= 0)
            highest, total, acc = state
            score = jnp.einsum("qhgd,khd->hgqk", query_block, key_block) * scale
            score = jnp.where(mask[None, None], score, -1e30)
            newmax = jnp.maximum(highest, jnp.max(score, axis=-1))
            factor = jnp.exp(highest - newmax)
            expo = jnp.exp(score - newmax[..., None])
            total = total * factor + jnp.sum(expo, axis=-1)
            rounded = lax.optimization_barrier(expo.astype(jnp.bfloat16)).astype(jnp.float32)
            acc = acc * factor[..., None] + jnp.einsum("hgqk,khd->hgqd", rounded, value_block)
            return newmax, total, acc

        def step(back, state):
            first = (start - back * block).astype(jnp.int32)
            last = first + block - 1
            need = (back == 0) | ((last >= 0) & (doc_index(jnp.maximum(last, 0)[None], ends)[0] == qdoc[0]))
            return lax.cond(need, lambda s: update(s, back), lambda s: s, state)

        init = (jnp.full((kvheads, group, block), -1e30, jnp.float32),
                jnp.zeros((kvheads, group, block), jnp.float32),
                jnp.zeros((kvheads, group, block, hdim), jnp.float32))
        highest, total, acc = lax.fori_loop(0, SPAN + 1, step, init)
        result = acc / total[..., None]
        return jnp.transpose(result, (2, 0, 1, 3)).reshape(block, qheads * hdim).astype(jnp.bfloat16)

    outs = lax.map(one_block, jnp.arange(tokens // block, dtype=jnp.int32))
    return outs.reshape(tokens, qheads * hdim)
```

```python
import functools
import math

import jax
import jax.numpy as jnp
from jax import lax
from jax.experimental import pallas as pl
from jax.experimental.pallas import tpu as pltpu
from jax.sharding import PartitionSpec as P

MESH = pl.DeviceIdType.MESH
BIG = 1e30
TILE = 512


def kernel(n, heads, lens_ref, q_ref, k_ref, v_ref, out_ref,
           kbuf, vbuf, kdoc, qaug, acc, top, norm, stage,
           send_sem, recv_sem, osend_sem, orecv_sem):
    rows, hdim = k_ref.shape
    total_rows = q_ref.shape[0]
    group = total_rows // rows
    me = lax.axis_index("ctx")
    mine = lax.axis_index("head")
    pos = me % 4
    core = pos % 2
    col = pos // 2
    mate = me + 1 - 2 * core
    across = me + 2 - 4 * col
    pos_m = pos + 1 - 2 * core
    pos_x = pos + 2 - 4 * col
    pos_d = pos_x + pos_m - pos
    has1 = me >= 4
    has2 = me >= 8
    feeds = me + 4 < n
    right = col == 1
    leftc = col == 0

    barrier = pltpu.get_barrier_semaphore()
    for peer in (mate, across):
        pl.semaphore_signal(barrier, inc=1, device_id={"ctx": peer}, device_id_type=MESH)

    @pl.when(has1)
    def _():
        pl.semaphore_signal(barrier, inc=1, device_id={"ctx": me - 4}, device_id_type=MESH)

    @pl.when(feeds)
    def _():
        pl.semaphore_signal(barrier, inc=1, device_id={"ctx": me + 4}, device_id_type=MESH)

    for d in range(1, heads):
        pl.semaphore_signal(barrier, inc=1, device_id={"head": (mine + d) % heads}, device_id_type=MESH)
    pl.semaphore_wait(barrier, 1 + heads + has1.astype(jnp.int32) + feeds.astype(jnp.int32))

    def copies(lane, slot, to_slot, target):
        made = []
        for w, buf, own in ((0, kbuf, k_ref), (1, vbuf, v_ref)):
            made.append(pltpu.make_async_remote_copy(
                src_ref=own if slot is None else buf.at[slot],
                dst_ref=buf.at[to_slot],
                send_sem=send_sem.at[lane, w],
                recv_sem=recv_sem.at[to_slot, w],
                device_id={"ctx": target},
                device_id_type=MESH,
            ))
        return made

    moves = {
        "D0": (copies(0, None, 8 + pos, mate), None),
        "X0": (copies(1, None, 8 + pos, across), leftc),
        "Z0": (copies(2, None, 4 + pos, me + 4), feeds),
        "D0x": (copies(3, 8 + pos_x, 8 + pos_x, mate), right),
        "D1": (copies(4, 4 + pos, 4 + pos, mate), has1),
        "X1": (copies(5, 4 + pos, 4 + pos, across), has1),
        "Z1": (copies(6, 4 + pos, pos, me + 4), has1 & feeds),
        "D1x": (copies(7, 4 + pos_x, 4 + pos_x, mate), has1),
        "D2": (copies(8, pos, pos, mate), has2),
        "X2": (copies(9, pos, pos, across), has2 & right),
        "D2x": (copies(10, pos_x, pos_x, mate), has2 & leftc),
    }

    def when(cond, fn):
        if cond is None:
            fn()
        else:
            pl.when(cond)(fn)

    def start(name):
        made, cond = moves[name]

        def go():
            for copy in made:
                copy.start()

        when(cond, go)

    def sent(name):
        made, cond = moves[name]

        def go():
            for copy in made:
                copy.wait_send()

        when(cond, go)

    def landed(slot, cond):
        def go():
            for w, buf in ((0, kbuf), (1, vbuf)):
                pltpu.make_async_copy(buf.at[slot], buf.at[slot], recv_sem.at[slot, w]).wait()

        when(cond, go)

    start("Z0")
    start("X0")
    start("D0")

    lane = lax.broadcasted_iota(jnp.int32, (8, 128), 1)
    firsts = jnp.full((8, 128), 2**30, jnp.int32)
    ends = jnp.full((8, 128), 2**30, jnp.int32)
    run = jnp.int32(0)
    for d in range(lens_ref.shape[0]):
        firsts = jnp.where(lane == d, run, firsts)
        run = run + lens_ref[d]
        ends = jnp.where(lane == d, run, ends)
    first_row, end_row = firsts[0:1], ends[0:1]

    def member(position):
        return (position >= first_row) & (position < end_row)

    base = me * rows

    @pl.loop(0, total_rows // TILE)
    def _(t):
        at = pl.ds(pl.multiple_of(t * TILE, TILE), TILE)
        token = (t * TILE + lax.broadcasted_iota(jnp.int32, (TILE, 128), 0)) // group
        qaug[at, 0:hdim] = q_ref[at, :]
        qaug[at, hdim:] = jnp.where(member(base + token), 1.0, 0.0).astype(jnp.bfloat16)

    @pl.loop(0, 12)
    def _(s):
        kpos = (me - pos - 8 + s) * rows + lax.broadcasted_iota(jnp.int32, (rows, 128), 0)
        kdoc[s] = jnp.where(member(kpos), 0.0, -BIG).astype(jnp.bfloat16)

    @pl.when(me < 8)
    def _():
        @pl.loop(0, 4)
        def _(s):
            kbuf[s] = jnp.zeros((rows, hdim), jnp.bfloat16)
            vbuf[s] = jnp.zeros((rows, hdim), jnp.bfloat16)

    scale = math.log2(math.e) / hdim**0.5
    ones = jnp.ones((rows, 128), jnp.bfloat16)

    def spread(x, width):
        return jnp.concatenate([x] * (width // 128), axis=1)

    def score(at, keys, docs):
        return lax.dot_general(
            qaug[at, :], jnp.concatenate([keys, docs], axis=1), (((1,), (1,)), ((), ())),
            preferred_element_type=jnp.float32) * scale

    @pl.loop(0, total_rows // TILE)
    def _(t):
        at = pl.ds(pl.multiple_of(t * TILE, TILE), TILE)
        s = score(at, k_ref[...], kdoc[8 + pos])
        token = (t * TILE + lax.broadcasted_iota(jnp.int32, (TILE, rows), 0)) // group
        s = jnp.where(lax.broadcasted_iota(jnp.int32, (TILE, rows), 1) <= token, s, -BIG)
        m = jnp.broadcast_to(jnp.max(s, axis=1, keepdims=True), (TILE, 128))
        p = jnp.exp2(s - spread(m, rows)).astype(jnp.bfloat16)
        top[at, :] = m
        acc[at, :] = jnp.dot(p, jnp.concatenate([v_ref[...], ones], axis=1),
                             preferred_element_type=jnp.float32)

    def both(at, a, b):
        keep = []
        sa = score(at, kbuf[a], kdoc[a])
        sb = score(at, kbuf[b], kdoc[b])
        m0 = top[at, :]
        m = jnp.maximum(m0, jnp.max(jnp.maximum(sa, sb), axis=1, keepdims=True))
        wide = spread(m, rows)
        pa = jnp.exp2(sa - wide).astype(jnp.bfloat16)
        pb = jnp.exp2(sb - wide).astype(jnp.bfloat16)
        top[at, :] = m
        grown = jnp.dot(pa, jnp.concatenate([vbuf[a], ones], axis=1), preferred_element_type=jnp.float32)
        grown = grown + jnp.dot(pb, jnp.concatenate([vbuf[b], ones], axis=1), preferred_element_type=jnp.float32)
        return acc[at, :] * spread(jnp.exp2(m0 - m), 256) + grown

    def pair(a, b, valid):
        @pl.when(valid)
        def _():
            @pl.loop(0, total_rows // TILE)
            def _(t):
                at = pl.ds(pl.multiple_of(t * TILE, TILE), TILE)
                acc[at, :] = both(at, a, b)

    def pick(if_right, if_left):
        return col * if_right + (1 - col) * if_left

    g1 = (4 + pos, 4 + pos_m)
    g2 = (4 + pos_x, 4 + pos_d)
    g3 = (pick(8 + pos_x, pos_x), pick(8 + pos_d, pos_d))
    g4 = (pos, core * (8 + pos_m) + (1 - core) * pos_m)

    landed(4 + pos, has1)
    start("Z1")
    start("X1")
    start("D1")
    landed(8 + pos_x, right)
    start("D0x")
    landed(8 + pos_m, None)
    landed(4 + pos_m, has1)
    landed(8 + pos_d, right)
    pair(pick(g3[0], g1[0]), pick(g3[1], g1[1]), right | has1)

    landed(pos, has2)
    start("X2")
    start("D2")
    landed(4 + pos_x, has1)
    start("D1x")
    landed(4 + pos_d, has1)
    pair(pick(g1[0], g2[0]), pick(g1[1], g2[1]), has1)

    landed(pos_m, has2)
    pair(pick(g2[0], g4[0]), pick(g2[1], g4[1]), (right & has1) | (leftc & (has2 | (core == 1))))

    landed(pos_x, has2 & leftc)
    start("D2x")
    landed(pos_d, has2 & leftc)
    last_a, last_b = pick(g4[0], g3[0]), pick(g4[1], g3[1])
    last_valid = has2 | (right & (core == 1))

    part = rows // heads
    tokens = TILE // group
    steps = part // tokens
    columns = pl.ds(pl.multiple_of(mine * (group * hdim), group * hdim), group * hdim)

    def finish(owner, t, own):
        at = pl.ds(pl.multiple_of(owner * (part * group) + t * TILE, TILE), TILE)

        @pl.when(last_valid)
        def _():
            whole = both(at, last_a, last_b)
            norm[...] = whole[:, 0:hdim] / whole[:, hdim:]

        @pl.when(jnp.logical_not(last_valid))
        def _():
            whole = acc[at, :]
            norm[...] = whole[:, 0:hdim] / whole[:, hdim:]

        local = pl.ds(pl.multiple_of(t * tokens, tokens), tokens)
        for g in range(group):
            piece = norm[pl.ds(g, tokens, stride=group), :].astype(jnp.bfloat16)
            if own is None:
                where = pl.ds(pl.multiple_of(mine * (group * hdim) + g * hdim, hdim), hdim)
                out_ref[local, where] = piece
            else:
                stage[own, local, g * hdim:(g + 1) * hdim] = piece

    def outgoing(d, t):
        local = pl.ds(pl.multiple_of(t * tokens, tokens), tokens)
        return pltpu.make_async_remote_copy(
            src_ref=stage.at[d - 1, local],
            dst_ref=out_ref.at[local, columns],
            send_sem=osend_sem.at[d - 1, t],
            recv_sem=orecv_sem.at[d - 1, t],
            device_id={"head": (mine + d) % heads},
            device_id_type=MESH,
        )

    for d in range(1, heads):
        @pl.loop(0, steps)
        def _(t):
            finish((mine + d) % heads, t, d - 1)
            outgoing(d, t).start()

    @pl.loop(0, steps)
    def _(t):
        finish(mine, t, None)

    for d in range(1, heads):
        @pl.loop(0, steps)
        def _(t):
            outgoing(d, t).wait_send()
            source = (mine + heads - d) % heads
            local = pl.ds(pl.multiple_of(t * tokens, tokens), tokens)
            cols = pl.ds(pl.multiple_of(source * (group * hdim), group * hdim), group * hdim)
            got = out_ref.at[local, cols]
            pltpu.make_async_copy(got, got, orecv_sem.at[d - 1, t]).wait()

    for name in moves:
        sent(name)


def on_device(mesh, queries, keys, values, doc_lengths):
    rows, group, hdim = queries.shape
    heads = mesh.shape["head"]
    n = mesh.shape["ctx"]
    bf16, f32 = jnp.bfloat16, jnp.float32
    part = rows // heads
    steps = part * group // TILE
    vmem = pl.BlockSpec(memory_space=pltpu.VMEM)
    return pl.pallas_call(
        functools.partial(kernel, n, heads),
        out_shape=jax.ShapeDtypeStruct((part, heads * group * hdim), bf16),
        in_specs=[pl.BlockSpec(memory_space=pltpu.SMEM), vmem, vmem, vmem],
        out_specs=vmem,
        scratch_shapes=[
            pltpu.VMEM((12, rows, hdim), bf16),
            pltpu.VMEM((12, rows, hdim), bf16),
            pltpu.VMEM((12, rows, 128), bf16),
            pltpu.VMEM((rows * group, hdim + 128), bf16),
            pltpu.VMEM((rows * group, hdim + 128), f32),
            pltpu.VMEM((rows * group, 128), f32),
            pltpu.VMEM((TILE, hdim), f32),
            pltpu.VMEM((heads - 1, part, group * hdim), bf16),
            pltpu.SemaphoreType.DMA((11, 2)),
            pltpu.SemaphoreType.DMA((12, 2)),
            pltpu.SemaphoreType.DMA((heads - 1, steps)),
            pltpu.SemaphoreType.DMA((heads - 1, steps)),
        ],
        compiler_params=pltpu.CompilerParams(
            collective_id=0, has_side_effects=True, vmem_limit_bytes=56 * 1024 * 1024),
    )(doc_lengths, queries.reshape(rows * group, hdim), keys.reshape(rows, hdim), values.reshape(rows, hdim))


def solution(mesh):
    placed = (P("ctx", "head", None), P("ctx", "head", None), P("ctx", "head", None), P())
    return jax.shard_map(
        functools.partial(on_device, mesh), mesh=mesh, in_specs=placed,
        out_specs=P(("ctx", "head"), None), check_vma=False
    )
```

```python
import functools
import math

import jax
import jax.numpy as jnp
from jax import lax
from jax.experimental import pallas as pl
from jax.experimental.pallas import tpu as pltpu
from jax.sharding import PartitionSpec as P

MESH = pl.DeviceIdType.MESH
BIG = 1e30
MOST = 1024


def kernel(n, heads, tile, lens_ref, q_ref, k_ref, v_ref, out_ref,
           kbuf, vbuf, kdoc, qaug, acc, top, norm, stage,
           send_sem, recv_sem, osend_sem, orecv_sem):
    rows, hdim = k_ref.shape
    total_rows = q_ref.shape[0]
    group = total_rows // rows
    me = lax.axis_index("ctx")
    mine = lax.axis_index("head")
    pos = me % 4
    core = pos % 2
    col = pos // 2
    mate = me + 1 - 2 * core
    across = me + 2 - 4 * col
    pos_m = pos + 1 - 2 * core
    pos_x = pos + 2 - 4 * col
    pos_d = pos_x + pos_m - pos
    has1 = me >= 4
    has2 = me >= 8
    feeds = me + 4 < n
    right = col == 1
    leftc = col == 0

    barrier = pltpu.get_barrier_semaphore()
    for peer in (mate, across):
        pl.semaphore_signal(barrier, inc=1, device_id={"ctx": peer}, device_id_type=MESH)

    @pl.when(has1)
    def _():
        pl.semaphore_signal(barrier, inc=1, device_id={"ctx": me - 4}, device_id_type=MESH)

    @pl.when(feeds)
    def _():
        pl.semaphore_signal(barrier, inc=1, device_id={"ctx": me + 4}, device_id_type=MESH)

    for d in range(1, heads):
        pl.semaphore_signal(barrier, inc=1, device_id={"head": (mine + d) % heads}, device_id_type=MESH)
    pl.semaphore_wait(barrier, 1 + heads + has1.astype(jnp.int32) + feeds.astype(jnp.int32))

    def copies(lane, slot, to_slot, target):
        made = []
        for w, buf, own in ((0, kbuf, k_ref), (1, vbuf, v_ref)):
            made.append(pltpu.make_async_remote_copy(
                src_ref=own if slot is None else buf.at[slot],
                dst_ref=buf.at[to_slot],
                send_sem=send_sem.at[lane, w],
                recv_sem=recv_sem.at[to_slot, w],
                device_id={"ctx": target},
                device_id_type=MESH,
            ))
        return made

    moves = {
        "D0": (copies(0, None, 8 + pos, mate), None),
        "X0": (copies(1, None, 8 + pos, across), leftc),
        "Z0": (copies(2, None, 4 + pos, me + 4), feeds),
        "D0x": (copies(3, 8 + pos_x, 8 + pos_x, mate), right),
        "D1": (copies(4, 4 + pos, 4 + pos, mate), has1),
        "X1": (copies(5, 4 + pos, 4 + pos, across), has1),
        "Z1": (copies(6, 4 + pos, pos, me + 4), has1 & feeds),
        "D1x": (copies(7, 4 + pos_x, 4 + pos_x, mate), has1),
        "D2": (copies(8, pos, pos, mate), has2),
        "X2": (copies(9, pos, pos, across), has2 & right),
        "D2x": (copies(10, pos_x, pos_x, mate), has2 & leftc),
    }

    def when(cond, fn):
        if cond is None:
            fn()
        else:
            pl.when(cond)(fn)

    def start(name):
        made, cond = moves[name]

        def go():
            for copy in made:
                copy.start()

        when(cond, go)

    def sent(name):
        made, cond = moves[name]

        def go():
            for copy in made:
                copy.wait_send()

        when(cond, go)

    def landed(slot, cond):
        def go():
            for w, buf in ((0, kbuf), (1, vbuf)):
                pltpu.make_async_copy(buf.at[slot], buf.at[slot], recv_sem.at[slot, w]).wait()

        when(cond, go)

    start("Z0")
    start("X0")
    start("D0")

    lane = lax.broadcasted_iota(jnp.int32, (8, 128), 1)
    firsts = jnp.full((8, 128), 2**30, jnp.int32)
    ends = jnp.full((8, 128), 2**30, jnp.int32)
    run = jnp.int32(0)
    for d in range(lens_ref.shape[0]):
        firsts = jnp.where(lane == d, run, firsts)
        run = run + lens_ref[d]
        ends = jnp.where(lane == d, run, ends)
    first_row, end_row = firsts[0:1], ends[0:1]

    def member(position):
        return (position >= first_row) & (position < end_row)

    base = me * rows

    @pl.loop(0, total_rows // tile)
    def _(t):
        at = pl.ds(pl.multiple_of(t * tile, tile), tile)
        token = (t * tile + lax.broadcasted_iota(jnp.int32, (tile, 128), 0)) // group
        qaug[at, 0:hdim] = q_ref[at, :]
        qaug[at, hdim:] = jnp.where(member(base + token), 1.0, 0.0).astype(jnp.bfloat16)

    @pl.loop(0, 12)
    def _(s):
        kpos = (me - pos - 8 + s) * rows + lax.broadcasted_iota(jnp.int32, (rows, 128), 0)
        kdoc[s] = jnp.where(member(kpos), 0.0, -BIG).astype(jnp.bfloat16)

    @pl.when(me < 8)
    def _():
        @pl.loop(0, 4)
        def _(s):
            kbuf[s] = jnp.zeros((rows, hdim), jnp.bfloat16)
            vbuf[s] = jnp.zeros((rows, hdim), jnp.bfloat16)

    scale = math.log2(math.e) / hdim**0.5

    def spread(x, width):
        return jnp.concatenate([x] * (width // 128), axis=1)

    def score(at, keys, docs):
        return lax.dot_general(
            qaug[at, :], jnp.concatenate([keys, docs], axis=1), (((1,), (1,)), ((), ())),
            preferred_element_type=jnp.float32) * scale

    @pl.loop(0, total_rows // tile)
    def _(t):
        at = pl.ds(pl.multiple_of(t * tile, tile), tile)
        s = score(at, k_ref[...], kdoc[8 + pos])
        token = (t * tile + lax.broadcasted_iota(jnp.int32, (tile, rows), 0)) // group
        s = jnp.where(lax.broadcasted_iota(jnp.int32, (tile, rows), 1) <= token, s, -BIG)
        m = jnp.broadcast_to(jnp.max(s, axis=1, keepdims=True), (tile, 128))
        e = jnp.exp2(s - spread(m, rows))
        top[at, :] = m
        acc[at, 0:128] = jnp.dot(e.astype(jnp.bfloat16), v_ref[...], preferred_element_type=jnp.float32)
        acc[at, 128:] = sum(e[:, k * 128:(k + 1) * 128] for k in range(rows // 128))

    def both(at, a, b):
        sa = score(at, kbuf[a], kdoc[a])
        sb = score(at, kbuf[b], kdoc[b])
        m0 = top[at, :]
        m = jnp.maximum(m0, jnp.max(jnp.maximum(sa, sb), axis=1, keepdims=True))
        wide = spread(m, rows)
        ea = jnp.exp2(sa - wide)
        eb = jnp.exp2(sb - wide)
        pa = ea.astype(jnp.bfloat16)
        pb = eb.astype(jnp.bfloat16)
        top[at, :] = m
        grown = jnp.dot(pa, vbuf[a], preferred_element_type=jnp.float32)
        grown = grown + jnp.dot(pb, vbuf[b], preferred_element_type=jnp.float32)
        factor = jnp.exp2(m0 - m)
        tot = sum(ea[:, k * 128:(k + 1) * 128] + eb[:, k * 128:(k + 1) * 128] for k in range(rows // 128))
        return jnp.concatenate([acc[at, 0:128] * factor + grown, acc[at, 128:] * factor + tot], axis=1)

    def pair(a, b, valid):
        @pl.when(valid)
        def _():
            @pl.loop(0, total_rows // tile)
            def _(t):
                at = pl.ds(pl.multiple_of(t * tile, tile), tile)
                acc[at, :] = both(at, a, b)

    def pick(if_right, if_left):
        return col * if_right + (1 - col) * if_left

    g1 = (4 + pos, 4 + pos_m)
    g2 = (4 + pos_x, 4 + pos_d)
    g3 = (pick(8 + pos_x, pos_x), pick(8 + pos_d, pos_d))
    g4 = (pos, core * (8 + pos_m) + (1 - core) * pos_m)

    landed(4 + pos, has1)
    start("Z1")
    start("X1")
    start("D1")
    landed(8 + pos_x, right)
    start("D0x")
    landed(8 + pos_m, None)
    landed(4 + pos_m, has1)
    landed(8 + pos_d, right)
    pair(pick(g3[0], g1[0]), pick(g3[1], g1[1]), right | has1)

    landed(pos, has2)
    start("X2")
    start("D2")
    landed(4 + pos_x, has1)
    start("D1x")
    landed(4 + pos_d, has1)
    pair(pick(g1[0], g2[0]), pick(g1[1], g2[1]), has1)

    landed(pos_m, has2)
    pair(pick(g2[0], g4[0]), pick(g2[1], g4[1]), (right & has1) | (leftc & (has2 | (core == 1))))

    landed(pos_x, has2 & leftc)
    start("D2x")
    landed(pos_d, has2 & leftc)
    last_a, last_b = pick(g4[0], g3[0]), pick(g4[1], g3[1])
    last_valid = has2 | (right & (core == 1))

    part = rows // heads
    tokens = tile // group
    steps = part // tokens
    columns = pl.ds(pl.multiple_of(mine * (group * hdim), group * hdim), group * hdim)

    def finish(owner, t, own):
        at = pl.ds(pl.multiple_of(owner * (part * group) + t * tile, tile), tile)

        @pl.when(last_valid)
        def _():
            whole = both(at, last_a, last_b)
            norm[...] = whole[:, 0:hdim] / jnp.sum(whole[:, hdim:], axis=1, keepdims=True)

        @pl.when(jnp.logical_not(last_valid))
        def _():
            whole = acc[at, :]
            norm[...] = whole[:, 0:hdim] / jnp.sum(whole[:, hdim:], axis=1, keepdims=True)

        local = pl.ds(pl.multiple_of(t * tokens, tokens), tokens)
        for g in range(group):
            piece = norm[pl.ds(g, tokens, stride=group), :].astype(jnp.bfloat16)
            if own is None:
                where = pl.ds(pl.multiple_of(mine * (group * hdim) + g * hdim, hdim), hdim)
                out_ref[local, where] = piece
            else:
                stage[own, local, g * hdim:(g + 1) * hdim] = piece

    def outgoing(d, t):
        local = pl.ds(pl.multiple_of(t * tokens, tokens), tokens)
        return pltpu.make_async_remote_copy(
            src_ref=stage.at[d - 1, local],
            dst_ref=out_ref.at[local, columns],
            send_sem=osend_sem.at[d - 1, t],
            recv_sem=orecv_sem.at[d - 1, t],
            device_id={"head": (mine + d) % heads},
            device_id_type=MESH,
        )

    for d in range(1, heads):
        @pl.loop(0, steps)
        def _(t):
            finish((mine + d) % heads, t, d - 1)
            outgoing(d, t).start()

    @pl.loop(0, steps)
    def _(t):
        finish(mine, t, None)

    for d in range(1, heads):
        @pl.loop(0, steps)
        def _(t):
            outgoing(d, t).wait_send()
            source = (mine + heads - d) % heads
            local = pl.ds(pl.multiple_of(t * tokens, tokens), tokens)
            cols = pl.ds(pl.multiple_of(source * (group * hdim), group * hdim), group * hdim)
            got = out_ref.at[local, cols]
            pltpu.make_async_copy(got, got, orecv_sem.at[d - 1, t]).wait()

    for name in moves:
        sent(name)


def on_device(mesh, queries, keys, values, doc_lengths):
    rows, group, hdim = queries.shape
    heads = mesh.shape["head"]
    n = mesh.shape["ctx"]
    bf16, f32 = jnp.bfloat16, jnp.float32
    part = rows // heads
    tile = min(MOST, part * group)
    steps = part * group // tile
    vmem = pl.BlockSpec(memory_space=pltpu.VMEM)
    return pl.pallas_call(
        functools.partial(kernel, n, heads, tile),
        out_shape=jax.ShapeDtypeStruct((part, heads * group * hdim), bf16),
        in_specs=[pl.BlockSpec(memory_space=pltpu.SMEM), vmem, vmem, vmem],
        out_specs=vmem,
        scratch_shapes=[
            pltpu.VMEM((12, rows, hdim), bf16),
            pltpu.VMEM((12, rows, hdim), bf16),
            pltpu.VMEM((12, rows, 128), bf16),
            pltpu.VMEM((rows * group, hdim + 128), bf16),
            pltpu.VMEM((rows * group, hdim + 128), f32),
            pltpu.VMEM((rows * group, 128), f32),
            pltpu.VMEM((tile, hdim), f32),
            pltpu.VMEM((heads - 1, part, group * hdim), bf16),
            pltpu.SemaphoreType.DMA((11, 2)),
            pltpu.SemaphoreType.DMA((12, 2)),
            pltpu.SemaphoreType.DMA((heads - 1, steps)),
            pltpu.SemaphoreType.DMA((heads - 1, steps)),
        ],
        compiler_params=pltpu.CompilerParams(
            collective_id=0, has_side_effects=True, vmem_limit_bytes=56 * 1024 * 1024),
    )(doc_lengths, queries.reshape(rows * group, hdim), keys.reshape(rows, hdim), values.reshape(rows, hdim))


def solution(mesh):
    placed = (P("ctx", "head", None), P("ctx", "head", None), P("ctx", "head", None), P())
    return jax.shard_map(
        functools.partial(on_device, mesh), mesh=mesh, in_specs=placed,
        out_specs=P(("ctx", "head"), None), check_vma=False
    )
```
